32 devices in a mesh: blk: 16 (over z, y, core), rep: 2 (over x).
Axes of the slice: x: 2, y: 2, z: 4, core: 2. Of those that a mesh axis runs over, the one named last changes fastest.
Arguments:
- queries: bfloat16 [4096, 1024], P('blk'), may hold values from -20 to 20
- corpus: bfloat16 [2, 32768, 1024], P('rep', 'blk'), may hold values from -5 to 5
- attributions: bfloat16 [2, 32768, 1024], P('rep', 'blk'), may hold values from -6 to 6
Outputs:
- attributed: bfloat16 [4096, 1024], P('blk')
- log_total: float32 [4096], P('blk')
The draws below stay inside these ranges and needn't reach their ends.
All inputs are finite; a program needn't handle non-finite values.
Results may differ from the reference program's by a relative error of at most 0.003.
Values may be sent and summed in bfloat16 or wider, within the bound.
No kernel may reach another device: no remote copies, remote signals or barrier semaphores. Data moves between devices by JAX's collectives and lax.ppermute only.
A program may use at most 64 MiB of HBM per device.

```python
import jax
import jax.numpy as jnp
from jax import lax

D = 1024
DV = 1024
Q_DEV = 256
C_DEV = 2048
STEPS = 4
QUERIES = 4096
SLAB_ROWS = 32768
N_BLK = 16
N_REP = 2


def corpus_base(key):
    return jax.random.truncated_normal(jax.random.fold_in(key, 11), -5.0, 5.0, (N_REP, SLAB_ROWS, D), jnp.float32)


def draw_corpus(key, part):
    base = corpus_base(key)
    return base.astype(jnp.bfloat16)


def draw_queries(key, part):
    noise = jax.random.truncated_normal(jax.random.fold_in(key, 23), -5.0, 5.0, (QUERIES, D), jnp.float32)
    return noise.astype(jnp.bfloat16)


def block_levels(rng, dims, cuts, least, top_value):
    def one(dim, shards_of):
        draws = jax.random.uniform(jax.random.fold_in(jax.random.fold_in(rng, 6), dim), (shards_of,), jnp.float32, least / len(cuts), top_value / len(cuts))
        return jnp.repeat(jnp.exp(draws), dims[dim] // shards_of).reshape((-1,) + (1,) * (len(dims) - dim - 1))

    loudness = one(*cuts[0])
    for cut in cuts[1:]:
        loudness = loudness * one(*cut)
    return loudness


def centred(own_key, extent, scale, reach, cuts=(), held_as=jnp.bfloat16):
    entries = scale * jax.random.normal(own_key, extent, jnp.float32)
    if cuts:
        entries = entries * block_levels(own_key, extent, cuts, -0.22, 0.18)
    return jnp.clip(entries, -reach, reach).astype(held_as)


def setup_inputs(seed: int = 0) -> dict:
    seeds = jax.random.split(jax.random.key(seed), 4)
    queries = draw_queries(jax.random.fold_in(seeds[3], 71), 0)
    corpus = draw_corpus(jax.random.fold_in(seeds[3], 71), 0)
    attributions = centred(seeds[2], (N_REP, SLAB_ROWS, DV), 1.0, 6.0, ((0, 2), (1, 16)))
    return dict(queries=queries, corpus=corpus, attributions=attributions)


sharpness = 2.5

def partial_stats(block_queries, slab_keys, slab_values):
    scores = jnp.dot(block_queries, slab_keys.T, preferred_element_type=jnp.float32) * (sharpness / jnp.sqrt(jnp.float32(block_queries.shape[1])))
    row_max = lax.optimization_barrier(jnp.max(scores, axis=1))
    weights = jnp.exp(scores - row_max[:, None])
    row_sum = lax.optimization_barrier(jnp.sum(weights, axis=1))
    weighted = jnp.dot(weights.astype(jnp.bfloat16), slab_values, preferred_element_type=jnp.float32)
    return (row_max, row_sum, weighted)

def combine(left_part, right_part):
    joined = jnp.maximum(left_part[0], right_part[0])
    left_factor = jnp.exp(left_part[0] - joined)
    right_factor = jnp.exp(right_part[0] - joined)
    row_sum = left_part[1] * left_factor + right_part[1] * right_factor
    weighted = left_part[2] * left_factor[:, None] + right_part[2] * right_factor[:, None]
    return (joined, row_sum, weighted)

def reference(queries, corpus, attributions):
    query_blocks = queries.reshape(N_BLK, Q_DEV, D)
    key_slabs = corpus.reshape(N_REP, N_BLK, C_DEV, D)
    value_slabs = attributions.reshape(N_REP, N_BLK, C_DEV, DV)

    def one_block(block_index):
        block_queries = lax.dynamic_index_in_dim(query_blocks, block_index, 0, keepdims=False)
        running = None
        for quarter in range(N_REP):
            for offset in range(STEPS):
                slab = ((block_index + offset) % N_BLK).astype(jnp.int32)
                slab_keys = lax.dynamic_index_in_dim(key_slabs[quarter], slab, 0, keepdims=False)
                slab_values = lax.dynamic_index_in_dim(value_slabs[quarter], slab, 0, keepdims=False)
                stats = partial_stats(block_queries, slab_keys, slab_values)
                running = stats if running is None else combine(running, stats)
        attributed = (running[2] / running[1][:, None]).astype(jnp.bfloat16)
        log_total = running[0] + jnp.log(running[1])
        return (attributed, log_total)
    attributed, log_total = lax.map(one_block, jnp.arange(N_BLK, dtype=jnp.int32))
    return (attributed.reshape(QUERIES, DV), log_total.reshape(QUERIES))
```

```python
import jax
import jax.numpy as jnp
from jax import lax
from jax.sharding import PartitionSpec as P

sharpness = 2.5


def partial_stats(block_queries, slab_keys, slab_values):
    scores = jnp.dot(block_queries, slab_keys.T, preferred_element_type=jnp.float32) * (
        sharpness / jnp.sqrt(jnp.float32(block_queries.shape[1]))
    )
    row_max = jnp.max(scores, axis=1, keepdims=True)
    weights = jnp.exp(scores - row_max)
    row_sum = jnp.sum(weights, axis=1, keepdims=True)
    weighted = jnp.dot(
        weights.astype(jnp.bfloat16), slab_values, preferred_element_type=jnp.float32
    )
    return weighted / row_sum, row_max + jnp.log(row_sum)


def joined(parts):
    top = parts[0][1]
    for _, level in parts[1:]:
        top = jnp.maximum(top, level)
    total = 0.0
    mean = 0.0
    for value, level in parts:
        share = jnp.exp(level - top)
        total = total + share
        mean = mean + value.astype(jnp.float32) * share
    return mean / total, top + jnp.log(total)


def packed(part):
    return part[0].astype(jnp.float16), part[1]


def shards(queries, corpus, attributions):
    keys = corpus[0]
    values = attributions[0]
    n = lax.axis_size("blk")
    two = [(b, (b + 2) % n) for b in range(n)]
    two_back = [(d, s) for s, d in two]
    fourth = [(b, (b + (3 if b % 2 else 1)) % n) for b in range(n)]
    fourth_back = [(d, s) for s, d in fourth]
    pair = [(b, b ^ 1) for b in range(n)]

    def move(tree, pairs, axis="blk"):
        return jax.tree.map(lambda x: lax.ppermute(x, axis, pairs), tree)

    near = move(queries, two)
    other = move(queries, fourth)
    far = move(near, pair)
    own = partial_stats(queries, keys, values)
    near_part = partial_stats(near, keys, values)
    far_part = packed(partial_stats(far, keys, values))
    other_part = packed(partial_stats(other, keys, values))
    other_back = move(other_part, fourth_back)
    far_back = move(far_part, pair)
    near_back = move(packed(joined([near_part, far_back])), two_back)
    mine = packed(joined([own, other_back, near_back]))
    theirs = move(mine, [(0, 1), (1, 0)], "rep")
    first = lax.axis_index("rep") == 0
    a = jax.tree.map(lambda x, y: jnp.where(first, x, y), mine, theirs)
    b = jax.tree.map(lambda x, y: jnp.where(first, y, x), mine, theirs)
    attributed, log_total = joined([a, b])
    return attributed.astype(jnp.bfloat16), log_total[:, 0]


def solution(mesh):
    return jax.shard_map(
        shards,
        mesh=mesh,
        in_specs=(P("blk", None), P("rep", "blk", None), P("rep", "blk", None)),
        out_specs=(P("blk", None), P("blk")),
        check_vma=False,
    )
```

```python
import jax
import jax.numpy as jnp
from jax import lax
from jax.sharding import PartitionSpec as P


sharpness = 2.5
SPLIT = (1, 1)


def after(value, *earlier):
    return lax.optimization_barrier((value, earlier))[0]


def plain_part(block_queries, keys, values):
    scores = (sharpness / block_queries.shape[1] ** 0.5) * jnp.dot(
        block_queries, keys.T, preferred_element_type=jnp.float32
    )
    top = jnp.max(scores, axis=1, keepdims=True)
    weights = jnp.exp(scores - top)
    total = jnp.sum(weights, axis=1, keepdims=True)
    weighted = jnp.dot(weights.astype(jnp.bfloat16), values, preferred_element_type=jnp.float32)
    return weighted / total, top + jnp.log(total)


def joined(all_parts):
    top = all_parts[0][1]
    for _, level in all_parts[1:]:
        top = jnp.maximum(top, level)
    total = 0.0
    mean = 0.0
    for value, level in all_parts:
        share = jnp.exp(level - top)
        total = total + share
        mean = mean + value.astype(jnp.float32) * share
    return mean / total, top + jnp.log(total)


def packed(part):
    return part[0].astype(jnp.float16), part[1]


def program(queries, corpus, attributions):
    n = lax.axis_size("blk")
    two = [(b, (b + 2) % n) for b in range(n)]
    two_back = [(d, s) for s, d in two]
    fourth = [(b, (b + (3 if b % 2 else 1)) % n) for b in range(n)]
    fourth_back = [(d, s) for s, d in fourth]
    pair = [(b, b ^ 1) for b in range(n)]
    first = lax.axis_index("rep") == 0

    def move(value, pairs, axis="blk"):
        return lax.ppermute(value, axis, pairs)

    def move_part(part, pairs, axis="blk"):
        mean, level = part
        return move(mean, pairs, axis), move(after(level, mean), pairs, axis)

    def edges(c):
        rows = queries.shape[0]
        return rows * sum(SPLIT[:c]) // sum(SPLIT), rows * sum(SPLIT[: c + 1]) // sum(SPLIT)

    def cut(tree, c):
        lo, hi = edges(c)
        return jax.tree.map(lambda a: a[lo:hi], tree)

    near_1 = move(cut(queries, 0), two)
    other = move(queries, fourth)
    near_2 = move(cut(queries, 1), two)
    keys, values = corpus[0], attributions[0]
    own = plain_part(queries, keys, values)

    def window(near):
        far = move(near, pair)
        both = plain_part(jnp.concatenate([near, far]), keys, values)
        near_part, far_part = (jax.tree.map(lambda a: a[at], both) for at in (slice(near.shape[0]), slice(near.shape[0], None)))
        far_back = move_part(packed(far_part), pair)
        mine = packed(joined([near_part, far_back]))
        return mine, move_part(mine, two_back)

    def exchange(all_parts):
        mine = packed(joined(all_parts))
        return mine, move_part(mine, [(0, 1), (1, 0)], "rep")

    def finish(outs, mine, theirs, c):
        a = jax.tree.map(lambda x, y: jnp.where(first, x, y), mine, theirs)
        b = jax.tree.map(lambda x, y: jnp.where(first, y, x), mine, theirs)
        attributed, log_total = joined([a, b])
        at = edges(c)[0]
        return (
            lax.dynamic_update_slice(outs[0], attributed.astype(jnp.bfloat16), (at, 0)),
            lax.dynamic_update_slice(outs[1], log_total[:, 0], (at,)),
        )

    mine_1, back_1 = window(after(near_1, own))
    other_part = plain_part(after(other, mine_1), keys, values)
    other_part = packed(other_part)
    other_back = move_part(other_part, fourth_back)
    mine_2, back_2 = window(after(near_2, other_part))
    own_1, theirs_1 = exchange([cut(own, 0), cut(other_back, 0), after(back_1, mine_2)])
    own_2, theirs_2 = exchange([cut(own, 1), cut(other_back, 1), after(back_2, own_1)])
    outs = (jnp.zeros(queries.shape, jnp.bfloat16), jnp.zeros(queries.shape[:1], jnp.float32))
    outs = finish(outs, own_1, after(theirs_1, own_2), 0)
    outs = finish(outs, own_2, theirs_2, 1)
    return outs


def solution(mesh):
    return jax.shard_map(
        program,
        mesh=mesh,
        in_specs=(P("blk", None), P("rep", "blk", None), P("rep", "blk", None)),
        out_specs=(P("blk", None), P("blk")),
        check_vma=False,
    )
```

```python
import jax
import jax.numpy as jnp
from jax import lax
from jax.sharding import PartitionSpec as P


sharpness = 2.5
SPLIT = (1, 1)


def after(value, *earlier):
    return lax.optimization_barrier((value, earlier))[0]


def plain_part(block_queries, keys, values):
    scores = (sharpness / block_queries.shape[1] ** 0.5) * jnp.dot(
        block_queries, keys.T, preferred_element_type=jnp.float32
    )
    top = jnp.max(scores, axis=1, keepdims=True)
    weights = jnp.exp(scores - top)
    total = jnp.sum(weights, axis=1, keepdims=True)
    weighted = jnp.dot(weights.astype(jnp.bfloat16), values, preferred_element_type=jnp.float32)
    return weighted / total, top + jnp.log(total)


def joined(all_parts):
    top = all_parts[0][1]
    for _, level in all_parts[1:]:
        top = jnp.maximum(top, level)
    total = 0.0
    mean = 0.0
    for value, level in all_parts:
        share = jnp.exp(level - top)
        total = total + share
        mean = mean + value.astype(jnp.float32) * share
    return mean / total, top + jnp.log(total)


def packed(part):
    return part[0].astype(jnp.float16), part[1]


def program(queries, corpus, attributions):
    n = lax.axis_size("blk")
    two = [(b, (b + 2) % n) for b in range(n)]
    two_back = [(d, s) for s, d in two]
    fourth = [(b, (b + (3 if b % 2 else 1)) % n) for b in range(n)]
    fourth_back = [(d, s) for s, d in fourth]
    pair = [(b, b ^ 1) for b in range(n)]

    def move(value, pairs, axis="blk"):
        return lax.ppermute(value, axis, pairs)

    def move_part(part, pairs, axis="blk"):
        mean, level = part
        mean_there = move(mean, pairs, axis)
        return mean_there, move(after(level[:, 0], mean), pairs, axis)[:, None]

    def edges(c):
        rows = queries.shape[0]
        return rows * sum(SPLIT[:c]) // sum(SPLIT), rows * sum(SPLIT[: c + 1]) // sum(SPLIT)

    def cut(tree, c):
        lo, hi = edges(c)
        return jax.tree.map(lambda a: a[lo:hi], tree)

    near_1 = move(cut(queries, 0), two)
    other = move(queries, fourth)
    near_2 = move(cut(queries, 1), two)
    keys, values = corpus[0], attributions[0]
    own = plain_part(queries, keys, values)

    def window(near):
        far = move(near, pair)
        both = plain_part(jnp.concatenate([near, far]), keys, values)
        near_part, far_part = (jax.tree.map(lambda a: a[at], both) for at in (slice(near.shape[0]), slice(near.shape[0], None)))
        far_back = move_part(packed(far_part), pair)
        mine = packed(joined([near_part, far_back]))
        return mine, move_part(mine, two_back)

    def exchange(all_parts):
        mine = packed(joined(all_parts))
        return mine, move_part(mine, [(0, 1), (1, 0)], "rep")

    def finish(outs, mine, theirs, c):
        attributed, log_total = joined([mine, theirs])
        at = edges(c)[0]
        return (
            lax.dynamic_update_slice(outs[0], attributed.astype(jnp.bfloat16), (at, 0)),
            lax.dynamic_update_slice(outs[1], log_total[:, 0], (at,)),
        )

    mine_1, back_1 = window(after(near_1, own))
    other_part = plain_part(after(other, mine_1), keys, values)
    other_part = packed(other_part)
    other_back = move_part(other_part, fourth_back)
    mine_2, back_2 = window(after(near_2, other_part))
    own_1, theirs_1 = exchange([cut(own, 0), cut(other_back, 0), after(back_1, mine_2)])
    own_2, theirs_2 = exchange([cut(own, 1), cut(other_back, 1), after(back_2, own_1)])
    outs = (queries, own[1][:, 0])
    outs = finish(outs, own_1, after(theirs_1, own_2), 0)
    outs = finish(outs, own_2, theirs_2, 1)
    return outs


def solution(mesh):
    return jax.shard_map(
        program,
        mesh=mesh,
        in_specs=(P("blk", None), P("rep", "blk", None), P("rep", "blk", None)),
        out_specs=(P("blk", None), P("blk")),
        check_vma=False,
    )
```

```python
import jax
import jax.numpy as jnp
from jax import lax
from jax.experimental import pallas as pl
from jax.experimental.pallas import tpu as pltpu
from jax.sharding import PartitionSpec as P


sharpness = 2.5
PIECES = 8
GRANT = 4 * 2**20
SPLIT = (1, 1)


def after(value, *earlier):
    return lax.optimization_barrier((value, earlier))[0]


def plain_part(block_queries, keys, values):
    scores = (sharpness / block_queries.shape[1] ** 0.5) * jnp.dot(
        block_queries, keys.T, preferred_element_type=jnp.float32
    )
    top = jnp.max(scores, axis=1, keepdims=True)
    weights = jnp.exp(scores - top)
    total = jnp.sum(weights, axis=1, keepdims=True)
    weighted = jnp.dot(weights.astype(jnp.bfloat16), values, preferred_element_type=jnp.float32)
    return weighted / total, top + jnp.log(total)


def parts_kernel(*refs):
    count = (len(refs) - 3) // 3
    queries, (keys_ref, values_ref), outs, scores_ref = (
        refs[:count],
        refs[count : count + 2],
        refs[count + 2 : -1],
        refs[-1],
    )
    block = jnp.concatenate([q[...] for q in queries]) if count > 1 else queries[0][...]
    scale = sharpness / block.shape[1] ** 0.5
    step = keys_ref.shape[0] // PIECES
    top = None
    for j in range(PIECES):
        at = slice(j * step, (j + 1) * step)
        scores = scale * lax.dot_general(
            block, keys_ref[at, :], (((1,), (1,)), ((), ())), preferred_element_type=jnp.float32
        )
        scores_ref[:, at] = scores
        highest = jnp.max(scores, axis=1, keepdims=True)
        top = highest if top is None else jnp.maximum(top, highest)
    total = 0.0
    weighted = 0.0
    for j in range(PIECES):
        at = slice(j * step, (j + 1) * step)
        weights = jnp.exp(scores_ref[:, at] - top)
        total = total + jnp.sum(weights, axis=1, keepdims=True)
        weighted = weighted + jnp.dot(
            weights.astype(jnp.bfloat16), values_ref[at, :], preferred_element_type=jnp.float32
        )
    mean = weighted / total
    level = jnp.transpose(jnp.broadcast_to(top + jnp.log(total), (block.shape[0], 128)))
    row = 0
    for k, q in enumerate(queries):
        rows = slice(row, row + q.shape[0])
        outs[2 * k][...] = mean[rows]
        outs[2 * k + 1][...] = level[0:8, rows]
        row = rows.stop


def parts(queries, keys, values):
    shapes = [
        jax.ShapeDtypeStruct(shape, jnp.float32)
        for q in queries
        for shape in ((q.shape[0], values.shape[1]), (8, q.shape[0]))
    ]
    rows = sum(q.shape[0] for q in queries)
    vmem = pl.BlockSpec(memory_space=pltpu.VMEM)
    out = pl.pallas_call(
        parts_kernel,
        out_shape=tuple(shapes),
        in_specs=[vmem] * (len(queries) + 2),
        out_specs=(vmem,) * len(shapes),
        scratch_shapes=[pltpu.VMEM((rows, keys.shape[0]), jnp.float32)],
        compiler_params=pltpu.CompilerParams(vmem_limit_bytes=GRANT),
        name="parts",
    )(*queries, keys, values)
    return [(out[2 * k], out[2 * k + 1][0][:, None]) for k in range(len(queries))]


def joined(all_parts):
    top = all_parts[0][1]
    for _, level in all_parts[1:]:
        top = jnp.maximum(top, level)
    total = 0.0
    mean = 0.0
    for value, level in all_parts:
        share = jnp.exp(level - top)
        total = total + share
        mean = mean + value.astype(jnp.float32) * share
    return mean / total, top + jnp.log(total)


def packed(part):
    return part[0].astype(jnp.float16), part[1]


def program(queries, corpus, attributions):
    n = lax.axis_size("blk")
    two = [(b, (b + 2) % n) for b in range(n)]
    two_back = [(d, s) for s, d in two]
    fourth = [(b, (b + (3 if b % 2 else 1)) % n) for b in range(n)]
    fourth_back = [(d, s) for s, d in fourth]
    pair = [(b, b ^ 1) for b in range(n)]

    def move(value, pairs, axis="blk"):
        return lax.ppermute(value, axis, pairs)

    def move_part(part, pairs, axis="blk"):
        mean, level = part
        mean_there = move(mean, pairs, axis)
        return mean_there, move(after(level[:, 0], mean), pairs, axis)[:, None]

    def edges(c):
        rows = queries.shape[0]
        return rows * sum(SPLIT[:c]) // sum(SPLIT), rows * sum(SPLIT[: c + 1]) // sum(SPLIT)

    def cut(tree, c):
        lo, hi = edges(c)
        return jax.tree.map(lambda a: a[lo:hi], tree)

    near_1 = move(cut(queries, 0), two)
    other = move(queries, fourth)
    near_2 = move(cut(queries, 1), two)
    keys, values = corpus[0], attributions[0]
    keys_1 = pltpu.with_memory_space_constraint(keys, pltpu.VMEM)
    values_1 = pltpu.with_memory_space_constraint(values, pltpu.VMEM)
    own = plain_part(queries, keys, values)

    def window(near):
        far = move(near, pair)
        near_part, far_part = parts([near, far], keys_1, values_1)
        far_back = move_part(packed(far_part), pair)
        mine = packed(joined([near_part, far_back]))
        return mine, move_part(mine, two_back)

    def exchange(all_parts):
        mine = packed(joined(all_parts))
        return mine, move_part(mine, [(0, 1), (1, 0)], "rep")

    def finish(outs, mine, theirs, c):
        attributed, log_total = joined([mine, theirs])
        at = edges(c)[0]
        return (
            lax.dynamic_update_slice(outs[0], attributed.astype(jnp.bfloat16), (at, 0)),
            lax.dynamic_update_slice(outs[1], log_total[:, 0], (at,)),
        )

    mine_1, back_1 = window(after(near_1, own))
    (other_part,) = parts([after(other, mine_1)], keys_1, values_1)
    other_part = packed(other_part)
    other_back = move_part(other_part, fourth_back)
    mine_2, back_2 = window(after(near_2, other_part))
    own_1, theirs_1 = exchange([cut(own, 0), cut(other_back, 0), after(back_1, mine_2)])
    own_2, theirs_2 = exchange([cut(own, 1), cut(other_back, 1), after(back_2, own_1)])
    outs = (queries, own[1][:, 0])
    outs = finish(outs, own_1, after(theirs_1, own_2), 0)
    outs = finish(outs, own_2, theirs_2, 1)
    return outs


def solution(mesh):
    return jax.shard_map(
        program,
        mesh=mesh,
        in_specs=(P("blk", None), P("rep", "blk", None), P("rep", "blk", None)),
        out_specs=(P("blk", None), P("blk")),
        check_vma=False,
    )
```

```python
import jax
import jax.numpy as jnp
from jax import lax
from jax.experimental import pallas as pl
from jax.experimental.pallas import tpu as pltpu
from jax.sharding import PartitionSpec as P


sharpness = 2.5
PIECES = 8
GRANT = 4 * 2**20
SPLIT = (1, 1)


def after(value, *earlier):
    return lax.optimization_barrier((value, earlier))[0]


def plain_part(block_queries, keys, values):
    scores = (sharpness / block_queries.shape[1] ** 0.5) * jnp.dot(
        block_queries, keys.T, preferred_element_type=jnp.float32
    )
    top = jnp.max(scores, axis=1, keepdims=True)
    weights = jnp.exp(scores - top)
    total = jnp.sum(weights, axis=1, keepdims=True)
    weighted = jnp.dot(weights.astype(jnp.bfloat16), values, preferred_element_type=jnp.float32)
    return weighted / total, top + jnp.log(total)


def parts_kernel(*refs):
    count = (len(refs) - 3) // 3
    queries, (keys_ref, values_ref), outs, scores_ref = (
        refs[:count],
        refs[count : count + 2],
        refs[count + 2 : -1],
        refs[-1],
    )
    block = jnp.concatenate([q[...] for q in queries]) if count > 1 else queries[0][...]
    scale = sharpness / block.shape[1] ** 0.5
    step = keys_ref.shape[0] // PIECES
    top = None
    for j in range(PIECES):
        at = slice(j * step, (j + 1) * step)
        scores = scale * lax.dot_general(
            block, keys_ref[at, :], (((1,), (1,)), ((), ())), preferred_element_type=jnp.float32
        )
        scores_ref[:, at] = scores
        highest = jnp.max(scores, axis=1, keepdims=True)
        top = highest if top is None else jnp.maximum(top, highest)
    total = 0.0
    weighted = 0.0
    for j in range(PIECES):
        at = slice(j * step, (j + 1) * step)
        weights = jnp.exp(scores_ref[:, at] - top)
        total = total + jnp.sum(weights, axis=1, keepdims=True)
        weighted = weighted + jnp.dot(
            weights.astype(jnp.bfloat16), values_ref[at, :], preferred_element_type=jnp.float32
        )
    mean = weighted / total
    level = jnp.transpose(jnp.broadcast_to(top + jnp.log(total), (block.shape[0], 128)))
    row = 0
    for k, q in enumerate(queries):
        rows = slice(row, row + q.shape[0])
        outs[2 * k][...] = mean[rows]
        outs[2 * k + 1][...] = level[0:8, rows]
        row = rows.stop


def parts(queries, keys, values):
    shapes = [
        jax.ShapeDtypeStruct(shape, jnp.float32)
        for q in queries
        for shape in ((q.shape[0], values.shape[1]), (8, q.shape[0]))
    ]
    rows = sum(q.shape[0] for q in queries)
    vmem = pl.BlockSpec(memory_space=pltpu.VMEM)
    out = pl.pallas_call(
        parts_kernel,
        out_shape=tuple(shapes),
        in_specs=[vmem] * (len(queries) + 2),
        out_specs=(vmem,) * len(shapes),
        scratch_shapes=[pltpu.VMEM((rows, keys.shape[0]), jnp.float32)],
        compiler_params=pltpu.CompilerParams(vmem_limit_bytes=GRANT),
        name="parts",
    )(*queries, keys, values)
    return [(out[2 * k], out[2 * k + 1][0][:, None]) for k in range(len(queries))]


def store(outs, shape, attributed, level, at):
    rows = attributed.shape[0]

    def kernel(attributed_ref, level_ref, *refs):
        out_ref, level_out_ref, sems = refs[-3:]
        copies = [
            pltpu.make_async_copy(attributed_ref, out_ref.at[pl.ds(at, rows), :], sems.at[0]),
            pltpu.make_async_copy(level_ref, level_out_ref.at[:, pl.ds(at, rows)], sems.at[1]),
        ]
        for copy in copies:
            copy.start()
        for copy in copies:
            copy.wait()

    vmem = pl.BlockSpec(memory_space=pltpu.VMEM)
    hbm = pl.BlockSpec(memory_space=pltpu.HBM)
    return pl.pallas_call(
        kernel,
        out_shape=(
            jax.ShapeDtypeStruct(shape, attributed.dtype),
            jax.ShapeDtypeStruct((1, shape[0]), level.dtype),
        ),
        in_specs=[vmem, vmem] + [hbm] * len(outs),
        out_specs=(hbm, hbm),
        scratch_shapes=[pltpu.SemaphoreType.DMA((2,))],
        input_output_aliases={2 + k: k for k in range(len(outs))},
        compiler_params=pltpu.CompilerParams(vmem_limit_bytes=GRANT),
        name="store",
    )(attributed, level, *outs)


def joined(all_parts):
    top = all_parts[0][1]
    for _, level in all_parts[1:]:
        top = jnp.maximum(top, level)
    total = 0.0
    mean = 0.0
    for value, level in all_parts:
        share = jnp.exp(level - top)
        total = total + share
        mean = mean + value.astype(jnp.float32) * share
    return mean / total, top + jnp.log(total)


def packed(part):
    return part[0].astype(jnp.float16), part[1]


def program(queries, corpus, attributions):
    n = lax.axis_size("blk")
    two = [(b, (b + 2) % n) for b in range(n)]
    two_back = [(d, s) for s, d in two]
    fourth = [(b, (b + (3 if b % 2 else 1)) % n) for b in range(n)]
    fourth_back = [(d, s) for s, d in fourth]
    pair = [(b, b ^ 1) for b in range(n)]

    def move(value, pairs, axis="blk"):
        return lax.ppermute(value, axis, pairs)

    def move_part(part, pairs, axis="blk"):
        mean, level = part
        mean_there = move(mean, pairs, axis)
        return mean_there, move(after(level[:, 0], mean), pairs, axis)[:, None]

    def edges(c):
        rows = queries.shape[0]
        return rows * sum(SPLIT[:c]) // sum(SPLIT), rows * sum(SPLIT[: c + 1]) // sum(SPLIT)

    def cut(tree, c):
        lo, hi = edges(c)
        return jax.tree.map(lambda a: a[lo:hi], tree)

    near_1 = move(cut(queries, 0), two)
    other = move(queries, fourth)
    near_2 = move(cut(queries, 1), two)
    keys, values = corpus[0], attributions[0]
    keys_1 = pltpu.with_memory_space_constraint(keys, pltpu.VMEM)
    values_1 = pltpu.with_memory_space_constraint(values, pltpu.VMEM)
    own = plain_part(queries, keys, values)

    def window(near):
        far = move(near, pair)
        near_part, far_part = parts([near, far], keys_1, values_1)
        far_back = move_part(packed(far_part), pair)
        mine = packed(joined([near_part, far_back]))
        return mine, move_part(mine, two_back)

    def exchange(all_parts):
        mine = packed(joined(all_parts))
        return mine, move_part(mine, [(0, 1), (1, 0)], "rep")

    def finish(outs, mine, theirs, c):
        attributed, log_total = joined([mine, theirs])
        at = edges(c)[0]
        shape = (queries.shape[0], attributed.shape[1])
        return store(outs, shape, attributed.astype(jnp.bfloat16), log_total[:, 0][None], at)

    mine_1, back_1 = window(after(near_1, own))
    (other_part,) = parts([after(other, mine_1)], keys_1, values_1)
    other_part = packed(other_part)
    other_back = move_part(other_part, fourth_back)
    mine_2, back_2 = window(after(near_2, other_part))
    own_1, theirs_1 = exchange([cut(own, 0), cut(other_back, 0), after(back_1, mine_2)])
    own_2, theirs_2 = exchange([cut(own, 1), cut(other_back, 1), after(back_2, own_1)])
    outs = ()
    outs = finish(outs, own_1, after(theirs_1, own_2), 0)
    outs = finish(outs, own_2, theirs_2, 1)
    return outs[0], outs[1][0]


def solution(mesh):
    return jax.shard_map(
        program,
        mesh=mesh,
        in_specs=(P("blk", None), P("rep", "blk", None), P("rep", "blk", None)),
        out_specs=(P("blk", None), P("blk")),
        check_vma=False,
    )
```

```python
import jax
import jax.numpy as jnp
from jax import lax
from jax.experimental import pallas as pl
from jax.experimental.pallas import tpu as pltpu
from jax.sharding import PartitionSpec as P


sharpness = 2.5
PIECES = 8
GRANT = 4 * 2**20
SPLIT = (1, 1)


def after(value, *earlier):
    return lax.optimization_barrier((value, earlier))[0]


def power_of(mean):
    peak = jnp.max(jnp.abs(mean), axis=1, keepdims=True)
    return jnp.floor(jnp.log2(jnp.maximum(peak, 2.0**-100))) - 13.0


def plain_part(block_queries, keys, values):
    scores = (sharpness / block_queries.shape[1] ** 0.5) * jnp.dot(
        block_queries, keys.T, preferred_element_type=jnp.float32
    )
    top = jnp.max(scores, axis=1, keepdims=True)
    weights = jnp.exp(scores - top)
    total = jnp.sum(weights, axis=1, keepdims=True)
    weighted = jnp.dot(weights.astype(jnp.bfloat16), values, preferred_element_type=jnp.float32)
    mean = weighted / total
    return mean, top + jnp.log(total), power_of(mean)


def parts_kernel(*refs):
    count = (len(refs) - 3) // 3
    queries, (keys_ref, values_ref), outs, scores_ref = (
        refs[:count],
        refs[count : count + 2],
        refs[count + 2 : -1],
        refs[-1],
    )
    block = jnp.concatenate([q[...] for q in queries]) if count > 1 else queries[0][...]
    scale = sharpness / block.shape[1] ** 0.5
    step = keys_ref.shape[0] // PIECES
    top = None
    for j in range(PIECES):
        at = slice(j * step, (j + 1) * step)
        scores = scale * lax.dot_general(
            block, keys_ref[at, :], (((1,), (1,)), ((), ())), preferred_element_type=jnp.float32
        )
        scores_ref[:, at] = scores
        highest = jnp.max(scores, axis=1, keepdims=True)
        top = highest if top is None else jnp.maximum(top, highest)
    total = 0.0
    weighted = 0.0
    for j in range(PIECES):
        at = slice(j * step, (j + 1) * step)
        weights = jnp.exp(scores_ref[:, at] - top)
        total = total + jnp.sum(weights, axis=1, keepdims=True)
        weighted = weighted + jnp.dot(
            weights.astype(jnp.bfloat16), values_ref[at, :], preferred_element_type=jnp.float32
        )
    mean = weighted / total
    power = power_of(mean)
    mean = mean * jnp.exp2(-power)
    across = lambda column: jnp.transpose(jnp.broadcast_to(column, (block.shape[0], 128)))[0:8]
    level, power = across(top + jnp.log(total)), across(power)
    stats = jnp.where(lax.broadcasted_iota(jnp.int32, level.shape, 0) == 0, level, power)
    row = 0
    for k, q in enumerate(queries):
        rows = slice(row, row + q.shape[0])
        outs[2 * k][...] = mean[rows]
        outs[2 * k + 1][...] = stats[:, rows]
        row = rows.stop


def parts(queries, keys, values):
    shapes = [
        jax.ShapeDtypeStruct(shape, jnp.float32)
        for q in queries
        for shape in ((q.shape[0], values.shape[1]), (8, q.shape[0]))
    ]
    rows = sum(q.shape[0] for q in queries)
    vmem = pl.BlockSpec(memory_space=pltpu.VMEM)
    out = pl.pallas_call(
        parts_kernel,
        out_shape=tuple(shapes),
        in_specs=[vmem] * (len(queries) + 2),
        out_specs=(vmem,) * len(shapes),
        scratch_shapes=[pltpu.VMEM((rows, keys.shape[0]), jnp.float32)],
        compiler_params=pltpu.CompilerParams(vmem_limit_bytes=GRANT),
        name="parts",
    )(*queries, keys, values)
    return [(out[2 * k], out[2 * k + 1]) for k in range(len(queries))]


def store(outs, shape, attributed, level, at):
    rows = attributed.shape[0]

    def kernel(attributed_ref, level_ref, *refs):
        out_ref, level_out_ref, sems = refs[-3:]
        copies = [
            pltpu.make_async_copy(attributed_ref, out_ref.at[pl.ds(at, rows), :], sems.at[0]),
            pltpu.make_async_copy(level_ref, level_out_ref.at[:, pl.ds(at, rows)], sems.at[1]),
        ]
        for copy in copies:
            copy.start()
        for copy in copies:
            copy.wait()

    vmem = pl.BlockSpec(memory_space=pltpu.VMEM)
    hbm = pl.BlockSpec(memory_space=pltpu.HBM)
    return pl.pallas_call(
        kernel,
        out_shape=(
            jax.ShapeDtypeStruct(shape, attributed.dtype),
            jax.ShapeDtypeStruct((1, shape[0]), level.dtype),
        ),
        in_specs=[vmem, vmem] + [hbm] * len(outs),
        out_specs=(hbm, hbm),
        scratch_shapes=[pltpu.SemaphoreType.DMA((2,))],
        input_output_aliases={2 + k: k for k in range(len(outs))},
        compiler_params=pltpu.CompilerParams(vmem_limit_bytes=GRANT),
        name="store",
    )(attributed, level, *outs)


def joined(all_parts, own=None):
    everything = [(mean, stats[0][:, None], stats[1][:, None]) for mean, stats in all_parts]
    everything += [own] if own else []
    top = power = None
    for _, level, part_power in everything:
        top = level if top is None else jnp.maximum(top, level)
        power = part_power if power is None else jnp.maximum(power, part_power)
    total = 0.0
    mean = 0.0
    for k, (value, level, part_power) in enumerate(everything):
        share = jnp.exp(level - top)
        total = total + share
        scale = part_power if k < len(all_parts) else 0.0
        mean = mean + value.astype(jnp.float32) * (share * jnp.exp2(scale - power))
    return mean / total, top + jnp.log(total), power


def packed(mean, level, power):
    at = lax.broadcasted_iota(jnp.int32, (2, mean.shape[0]), 0)
    stats = jnp.where(at == 0, level[:, 0][None], power[:, 0][None])
    return mean.astype(jnp.float16), stats


def program(queries, corpus, attributions):
    n = lax.axis_size("blk")
    two = [(b, (b + 2) % n) for b in range(n)]
    two_back = [(d, s) for s, d in two]
    fourth = [(b, (b + (3 if b % 2 else 1)) % n) for b in range(n)]
    fourth_back = [(d, s) for s, d in fourth]
    pair = [(b, b ^ 1) for b in range(n)]

    def move(value, pairs, axis="blk"):
        return lax.ppermute(value, axis, pairs)

    def move_part(part, pairs, axis="blk"):
        mean, stats = part
        return move(mean, pairs, axis), move(after(stats, mean), pairs, axis)

    def edges(c):
        rows = queries.shape[0]
        return rows * sum(SPLIT[:c]) // sum(SPLIT), rows * sum(SPLIT[: c + 1]) // sum(SPLIT)

    def cut(tree, c):
        lo, hi = edges(c)
        return jax.tree.map(lambda a: a[lo:hi], tree)

    near_1 = move(cut(queries, 0), two)
    other = move(queries, fourth)
    near_2 = move(cut(queries, 1), two)
    keys, values = corpus[0], attributions[0]
    keys_1 = pltpu.with_memory_space_constraint(keys, pltpu.VMEM)
    values_1 = pltpu.with_memory_space_constraint(values, pltpu.VMEM)
    own = plain_part(queries, keys, values)

    def window(near):
        far = move(near, pair)
        near_part, far_part = parts([near, far], keys_1, values_1)
        far_back = move_part((far_part[0].astype(jnp.float16), far_part[1]), pair)
        mine = packed(*joined([near_part, far_back]))
        return mine, move_part(mine, two_back)

    def cut_part(part, c):
        lo, hi = edges(c)
        return part[0][lo:hi], part[1][:, lo:hi]

    def exchange(all_parts, own):
        mine = packed(*joined(all_parts, own))
        return mine, move_part(mine, [(0, 1), (1, 0)], "rep")

    def finish(outs, mine, theirs, c):
        mean, log_total, power = joined([mine, theirs])
        attributed = mean * jnp.exp2(power)
        at = edges(c)[0]
        shape = (queries.shape[0], attributed.shape[1])
        return store(outs, shape, attributed.astype(jnp.bfloat16), log_total[:, 0][None], at)

    mine_1, back_1 = window(after(near_1, own))
    (other_part,) = parts([after(other, mine_1)], keys_1, values_1)
    other_part = other_part[0].astype(jnp.float16), other_part[1]
    other_back = move_part(other_part, fourth_back)
    mine_2, back_2 = window(after(near_2, other_part))
    own_1, theirs_1 = exchange([cut_part(other_back, 0), after(back_1, mine_2)], cut(own, 0))
    own_2, theirs_2 = exchange([cut_part(other_back, 1), after(back_2, own_1)], cut(own, 1))
    outs = ()
    outs = finish(outs, own_1, after(theirs_1, own_2), 0)
    outs = finish(outs, own_2, theirs_2, 1)
    return outs[0], outs[1][0]


def solution(mesh):
    return jax.shard_map(
        program,
        mesh=mesh,
        in_specs=(P("blk", None), P("rep", "blk", None), P("rep", "blk", None)),
        out_specs=(P("blk", None), P("blk")),
        check_vma=False,
    )
```
